32 devices in a mesh: graph: 16 (over z, y, x), feat: 2 (over core).
Axes of the slice: x: 2, y: 2, z: 4, core: 2. Of those that a mesh axis runs over, the one named last changes fastest.
Arguments:
- features: bfloat16 [16384, 1024], P('graph', 'feat'), may hold values from -6 to 6
- rel_weight: bfloat16 [8, 1024, 1024], P(None, 'feat'), may hold values from -0.1875 to 0.1875
- self_weight: bfloat16 [1024, 1024], P('feat'), may hold values from -0.1875 to 0.1875
- type_bias: float32 [4, 1024], P(None, 'feat'), may hold values from -3 to 3
- node_type: int32 [16384], P('graph'), may hold values from 0 to 3
- tile_coef: bfloat16 [640, 128, 128], P('graph'), may hold values from -0.375 to 0.375
- tile_source: int32 [16, 40], P('graph'), may hold values from 0 to 23, as said below
- tile_target: int32 [16, 40], P('graph'), may hold values from 0 to 7
- tile_relation: int32 [16, 40], P('graph'), may hold values from 0 to 7
- send_block: int32 [16, 16], P('graph'), may hold values from 0 to 7
- send_live: int32 [16, 16], P('graph'), may hold values from 0 to 1, as said below
Outputs:
- updated: bfloat16 [16384, 1024], P('graph', 'feat')
The draws below stay inside these ranges and needn't reach their ends.
Inputs may be any that keep to these rules, and one draw needn't show every extreme that they name: send_live[s, s] is 0; partition q receives from 3 to 12 live blocks. `tile_source`: entries below 8 name the partition's own blocks; entry 8 + s names the block received from partition s and stands only where send_live[s, p] is 1; every live received block is named by some tile.
All inputs are finite; a program needn't handle non-finite values.
Results may differ from the reference program's by a relative error of at most 0.0065.
Values may be sent and summed in bfloat16 or wider, within the bound.
A program may use at most 64 MiB of HBM per device.

```python
import jax
import jax.numpy as jnp
from jax import lax

D = 1024
RELS = 8
NODE_TYPES = 4
BLOCK = 128
NODES_DEV = 1024
NODES = 16384
TILES_DEV = 40
N_GRAPH = 16


def boundary_plan(key):
    base = jax.random.fold_in(key, 7001)
    keys = jax.random.split(base, N_GRAPH)
    orders = jax.vmap(lambda k: jax.random.permutation(k, N_GRAPH))(keys)
    counts = jax.random.randint(jax.random.fold_in(key, 7002), (N_GRAPH,), N_GRAPH // 4, 3 * N_GRAPH // 4 + 1)
    ranks = jnp.argsort(orders, axis=1, stable=True)
    receivers = jnp.arange(N_GRAPH)[:, None]
    others = jnp.arange(N_GRAPH)[None, :]
    live_by_receiver = (ranks < counts[:, None]) & (others != receivers)
    return (orders, counts, live_by_receiver)


def draw_send_live(key, part):
    orders, counts, live_by_receiver = boundary_plan(key)
    return live_by_receiver.T.astype(jnp.int32)


def draw_tile_source(key, part):
    orders, counts, live_by_receiver = boundary_plan(key)
    count_blocks = NODES_DEV // BLOCK
    position = jnp.arange(TILES_DEV)[None, :]
    clamped = jnp.minimum(position, N_GRAPH - 1)
    sender = jnp.take_along_axis(orders, jnp.broadcast_to(clamped, (N_GRAPH, TILES_DEV)), axis=1)
    receivers = jnp.arange(N_GRAPH)[:, None]
    use_remote = (position < counts[:, None]) & (sender != receivers)
    local = jax.random.randint(jax.random.fold_in(key, 7003), (N_GRAPH, TILES_DEV), 0, count_blocks)
    return jnp.where(use_remote, count_blocks + sender, local).astype(jnp.int32)


def with_ends(values, own_key, low, high):
    index_at = [jax.random.randint(jax.random.fold_in(own_key, axis), (), 0, length) for axis, length in enumerate(values.shape)]
    widest = values.shape.index(max(values.shape))
    beside = index_at[:widest] + [(index_at[widest] + 1) % values.shape[widest]] + index_at[widest + 1:]
    return values.at[tuple(index_at)].set(low).at[tuple(beside)].set(high)


def level_of(rng, shape, pieces, smallest, largest):
    gain, own = 1.0, jax.random.fold_in(rng, 6)
    for dim, blocks in pieces:
        draws = jnp.exp(jax.random.uniform(jax.random.fold_in(own, dim), (blocks,), jnp.float32, smallest / len(pieces), largest / len(pieces)))
        gain = gain * jnp.repeat(draws, shape[dim] // blocks).reshape([-1 if axis == dim else 1 for axis in range(len(shape))])
    return gain


def scatter_about(stream_key, extent, width, bound, cuts=(), held_as=jnp.bfloat16):
    loudness = level_of(stream_key, extent, cuts, -0.22, 0.18) if cuts else 1.0
    entries = jax.random.normal(stream_key, extent, jnp.float32) * width * loudness
    return jnp.minimum(jnp.maximum(entries, -bound), bound).astype(held_as)


def setup_inputs(seed: int = 0) -> dict:
    arg_keys = jax.random.split(jax.random.key(seed), 12)
    features = scatter_about(arg_keys[0], (NODES, D), 1.0, 6.0, ((0, 16), (1, 2)))
    rel_weight = scatter_about(arg_keys[1], (RELS, D, D), D ** -0.5, 0.1875, ((1, 2),))
    self_weight = scatter_about(arg_keys[2], (D, D), D ** -0.5, 0.1875, ((0, 2),))
    type_bias = scatter_about(arg_keys[3], (NODE_TYPES, D), 0.5, 3.0, ((1, 2),), jnp.float32)
    node_type = with_ends(jax.random.randint(arg_keys[4], (NODES,), 0, NODE_TYPES), jax.random.fold_in(arg_keys[4], 1), 0, NODE_TYPES - 1).astype(jnp.int32)
    tile_coef = scatter_about(arg_keys[5], (N_GRAPH * TILES_DEV, BLOCK, BLOCK), (2 * BLOCK) ** -0.5, 0.375, ((0, 16),))
    tile_source = draw_tile_source(jax.random.fold_in(arg_keys[11], 71), 0)
    tile_target = with_ends(jax.random.randint(arg_keys[7], (N_GRAPH, TILES_DEV), 0, NODES_DEV // BLOCK), jax.random.fold_in(arg_keys[7], 1), 0, (NODES_DEV // BLOCK) - 1).astype(jnp.int32)
    tile_relation = with_ends(jax.random.randint(arg_keys[8], (N_GRAPH, TILES_DEV), 0, RELS), jax.random.fold_in(arg_keys[8], 1), 0, RELS - 1).astype(jnp.int32)
    send_block = with_ends(jax.random.randint(arg_keys[9], (N_GRAPH, N_GRAPH), 0, NODES_DEV // BLOCK), jax.random.fold_in(arg_keys[9], 1), 0, (NODES_DEV // BLOCK) - 1).astype(jnp.int32)
    send_live = draw_send_live(jax.random.fold_in(arg_keys[11], 71), 0)
    return {"features": features, "rel_weight": rel_weight, "self_weight": self_weight, "type_bias": type_bias, "node_type": node_type, "tile_coef": tile_coef, "tile_source": tile_source, "tile_target": tile_target, "tile_relation": tile_relation, "send_block": send_block, "send_live": send_live}


def reference(features, rel_weight, self_weight, type_bias, node_type, tile_coef, tile_source, tile_target, tile_relation, send_block, send_live):
    count_blocks = NODES_DEV // BLOCK
    blocked = features.reshape(N_GRAPH, count_blocks, BLOCK, D)
    coef_all = tile_coef.reshape(N_GRAPH, TILES_DEV, BLOCK, BLOCK)
    senders = jnp.arange(N_GRAPH, dtype=jnp.int32)
    kinds = jnp.arange(NODE_TYPES, dtype=jnp.int32)
    slots = jnp.arange(RELS * count_blocks, dtype=jnp.int32)

    def one_part(part):
        local = blocked[part]
        picks = send_block[:, part].astype(jnp.int32)
        remote = blocked[senders, picks] * send_live[:, part].astype(features.dtype)[:, None, None]
        table = jnp.concatenate([local, remote], axis=0)
        sources = table[tile_source[part].astype(jnp.int32)]
        products = jnp.einsum("tij,tjd->tid", coef_all[part].astype(jnp.float32), sources.astype(jnp.float32), precision=lax.Precision.HIGHEST)
        slot = tile_relation[part] * count_blocks + tile_target[part]
        onehot = (slot[:, None] == slots[None, :]).astype(jnp.float32)
        summed = jnp.einsum("tk,tbd->kbd", onehot, products, precision=lax.Precision.HIGHEST)
        aggregate = summed.reshape(RELS, NODES_DEV, D).astype(jnp.bfloat16)
        rows = local.reshape(NODES_DEV, D)
        partial_value = jnp.dot(rows, self_weight, preferred_element_type=jnp.float32)
        for relation in range(RELS):
            partial_value = partial_value + jnp.dot(aggregate[relation], rel_weight[relation], preferred_element_type=jnp.float32)
        types = lax.dynamic_slice(node_type, (part * NODES_DEV,), (NODES_DEV,))
        type_onehot = (types[:, None] == kinds[None, :]).astype(jnp.float32)
        biased = partial_value + jnp.dot(type_onehot, type_bias, precision=lax.Precision.HIGHEST)
        return jnp.maximum(biased, 0.0).astype(jnp.bfloat16)

    updated = lax.map(one_part, jnp.arange(N_GRAPH, dtype=jnp.int32))
    return updated.reshape(NODES, D)
```

```python
import functools

import jax
import jax.numpy as jnp
from jax import lax
from jax.experimental import pallas as pl
from jax.experimental.pallas import tpu as pltpu
from jax.sharding import PartitionSpec as P

MESH = pl.DeviceIdType.MESH
VMEM = 67_043_328


def partner(me, step, count):
    other, bit = 0, 1
    while bit < count:
        other = other + ((me // bit + step // bit) % 2) * bit
        bit *= 2
    return other


def exchange_kernel(
    groups,
    shards,
    block,
    send_block,
    send_live,
    tile_source,
    tile_target,
    tile_relation,
    source_row,
    target_row,
    bias_ref,
    type_ref,
    x_hbm,
    rel_ref,
    self_ref,
    coef_hbm,
    received,
    w_out,
    pre_out,
    outgoing,
    x_own,
    x_far,
    w_all,
    s_vmem,
    coef,
    sums,
    landed,
    far,
    pre,
    plan_vmem,
    plan,
    send_sem,
    recv_sem,
    pass_send,
    pass_recv,
    side_send,
    side_recv,
    local_sem,
    keep_sem,
    far_sem,
    out_sem,
):
    me, mine = lax.axis_index("graph"), lax.axis_index("feat")
    blocks, _, width = x_own.shape
    relations = rel_ref.shape[0]
    tiles = coef.shape[0]

    def columns(shard):
        return pl.ds(pl.multiple_of(shard * width, width), width)

    barrier = pltpu.get_barrier_semaphore()

    def greet(step, carry):
        pl.semaphore_signal(
            barrier, inc=1, device_id=(partner(me, step, groups), mine), device_id_type=MESH
        )
        return carry

    lax.fori_loop(1, groups, greet, 0)
    for e in range(1, shards):
        pl.semaphore_signal(
            barrier, inc=1, device_id=(me, (mine + e) % shards), device_id_type=MESH
        )

    x_copy = pltpu.make_async_copy(x_hbm, x_own, local_sem.at[3])
    own_rel = pltpu.make_async_copy(
        rel_ref.at[:, :, columns(mine)], w_all.at[mine, pl.ds(0, relations)], local_sem.at[0]
    )
    own_self = pltpu.make_async_copy(
        self_ref.at[:, columns(mine)], w_all.at[mine, relations], local_sem.at[1]
    )
    coef_copy = pltpu.make_async_copy(coef_hbm, coef, local_sem.at[4])
    x_copy.start()
    own_rel.start()
    own_self.start()
    coef_copy.start()
    x_copy.wait()

    def gather(q, carry):
        picked = x_own[send_block[0, q]].astype(jnp.float32)
        outgoing[q] = (picked * send_live[0, q].astype(jnp.float32)).astype(outgoing.dtype)
        return carry

    lax.fori_loop(0, groups, gather, 0)

    def iota(shape, axis):
        return lax.broadcasted_iota(jnp.int32, shape, axis)

    square = (tiles, tiles)
    down, along = iota(square, 0), iota(square, 1)

    def column(row):
        return jnp.sum(
            jnp.where(down == along, jnp.broadcast_to(row, square), 0), axis=1, keepdims=True
        )

    sources = column(source_row[...])
    keys_row = jnp.where(source_row[...] < blocks, target_row[...], blocks)
    keys = column(keys_row)
    ahead = (keys_row < keys) | ((keys_row == keys) & (along < down))
    rank = jnp.sum(ahead.astype(jnp.int32), axis=1, keepdims=True)
    plan_vmem[0:1, 0:tiles] = jnp.sum(
        jnp.where(rank == along, down, 0), axis=0, keepdims=True
    )
    wide = (tiles, groups)
    plan_vmem[1:2, 0:groups] = jnp.min(
        jnp.where(sources == blocks + iota(wide, 1), iota(wide, 0), tiles), axis=0, keepdims=True
    )
    each = (tiles, blocks)
    plan_vmem[2:3, 0:blocks] = jnp.sum(
        (keys <= iota(each, 1)).astype(jnp.int32), axis=0, keepdims=True
    )
    plan_vmem[3:4, 0:blocks] = jnp.sum(
        (keys == iota(each, 1)).astype(jnp.int32), axis=0, keepdims=True
    )
    plan_copy = pltpu.make_async_copy(plan_vmem, plan, local_sem.at[5])
    with jax.named_scope("barrier"):
        pl.semaphore_wait(barrier, groups - 1 + shards - 1)

    def boundary(step):
        other = partner(me, step, groups)
        return pltpu.make_async_remote_copy(
            src_ref=outgoing.at[other],
            dst_ref=landed.at[me],
            send_sem=send_sem.at[step],
            recv_sem=recv_sem.at[step],
            device_id=(other, mine),
            device_id_type=MESH,
        )

    half = groups // 2
    inner = (me // half + me // max(half // 2, 1)) % 2

    def send(i, carry):
        boundary(1 + (i + inner * (half - 1)) % (groups - 1)).start()
        return carry

    lax.fori_loop(0, groups - 1, send, 0)
    plan_copy.start()

    def side(e):
        peer = (mine + e) % shards
        pairs = (
            (x_own, x_far.at[mine]),
            (self_ref.at[:, columns(peer)], w_all.at[mine, relations]),
            (rel_ref.at[:, :, columns(peer)], w_all.at[mine, pl.ds(0, relations)]),
        )
        return [
            pltpu.make_async_remote_copy(
                src_ref=src,
                dst_ref=dst,
                send_sem=side_send.at[e - 1, i],
                recv_sem=side_recv.at[e - 1, i],
                device_id=(me, peer),
                device_id_type=MESH,
            )
            for i, (src, dst) in enumerate(pairs)
        ]

    sides = [copy for e in range(1, shards) for copy in side(e)]
    for copy in sides:
        copy.start()
    own_rel.wait()
    own_self.wait()
    with jax.named_scope("sides"):
        for copy in sides:
            copy.wait()
    w_copy = pltpu.make_async_copy(
        w_all.at[:, pl.ds(0, relations)], w_out, local_sem.at[2]
    )
    w_copy.start()

    chunk = 2

    def full_dot(start, relation):
        at = pl.ds(start, chunk)
        total = jnp.dot(
            x_own[at].reshape(chunk * block, width),
            w_all[mine, relation],
            preferred_element_type=jnp.float32,
        )
        for e in range(1, shards):
            peer = (mine + e) % shards
            total = total + jnp.dot(
                x_far[peer, at].reshape(chunk * block, width),
                w_all[peer, relation],
                preferred_element_type=jnp.float32,
            )
        return total.reshape(chunk, block, width)

    def own_part(i, carry):
        s_vmem[pl.ds(i * chunk, chunk)] = full_dot(i * chunk, relations)
        return carry

    with jax.named_scope("self"):
        lax.fori_loop(0, blocks // chunk, own_part, 0)

    coef_copy.wait()
    plan_copy.wait()
    stride = 4 if tiles % 4 == 0 else 1

    def local(i, carry):
        terms = []
        for j in range(stride):
            t = plan[0, i * stride + j]
            relation = tile_relation[0, t]
            source = jnp.minimum(tile_source[0, t], blocks - 1)
            value = jnp.dot(
                x_own[source], w_all[mine, relation], preferred_element_type=jnp.float32
            )
            for e in range(1, shards):
                peer = (mine + e) % shards
                value = value + jnp.dot(
                    x_far[peer, source], w_all[peer, relation], preferred_element_type=jnp.float32
                )
            terms.append((t, value.astype(coef.dtype)))
        for j, (t, value) in enumerate(terms):
            at = i * stride + j
            before = plan[0, jnp.maximum(at - 1, 0)]
            joins = (tile_target[0, t] == tile_target[0, before]) & (at > 0)
            term = jnp.dot(coef[t], value, preferred_element_type=jnp.float32)
            sums[at] = term + jnp.where(joins, sums[jnp.maximum(at - 1, 0)], 0.0)
        return carry

    with jax.named_scope("local"):
        lax.fori_loop(0, tiles // stride, local, 0)

    with jax.named_scope("base"):
        for i in range(blocks):
            kinds = jnp.transpose(jnp.broadcast_to(type_ref[i : i + 1, :], (block, block)))
            kinds = jnp.concatenate([kinds] * (width // block), axis=1)
            total = s_vmem[i]
            for kind in range(bias_ref.shape[0]):
                total = total + jnp.where(kinds == kind, bias_ref[kind : kind + 1, :], 0.0)
            last = jnp.maximum(plan[2, i] - 1, 0)
            s_vmem[i] = total + jnp.where(plan[3, i] > 0, sums[last], 0.0)

    def forward(step, e):
        other = partner(me, step, groups)
        return pltpu.make_async_remote_copy(
            src_ref=landed.at[other],
            dst_ref=far.at[mine, other],
            send_sem=pass_send.at[e - 1, step],
            recv_sem=pass_recv.at[e - 1, step],
            device_id=(me, (mine + e) % shards),
            device_id_type=MESH,
        )

    def keep(step):
        other = partner(me, step, groups)
        return pltpu.make_async_copy(
            landed.at[other], received.at[mine, other], keep_sem.at[step]
        )

    def keep_far(step, e):
        origin, other = (mine + shards - e) % shards, partner(me, step, groups)
        return pltpu.make_async_copy(
            far.at[origin, other], received.at[origin, other], far_sem.at[e - 1, step]
        )

    def arrived(step, carry):
        boundary(step).wait_recv()
        for e in range(1, shards):
            forward(step, e).start()
        keep(step).start()
        return carry

    def moved(step):
        other = partner(me, step, groups)
        found = plan[1, other]
        t = jnp.minimum(found, tiles - 1)
        relation = tile_relation[0, t]
        value = jnp.dot(
            landed[other], w_all[mine, relation], preferred_element_type=jnp.float32
        )
        for e in range(1, shards):
            origin = (mine + shards - e) % shards
            pltpu.make_async_remote_copy(
                src_ref=far.at[origin, other],
                dst_ref=far.at[origin, other],
                send_sem=pass_send.at[e - 1, step],
                recv_sem=pass_recv.at[e - 1, step],
                device_id=(me, (mine + e) % shards),
                device_id_type=MESH,
            ).wait_recv()
            keep_far(step, e).start()
            value = value + jnp.dot(
                far[origin, other], w_all[origin, relation], preferred_element_type=jnp.float32
            )
        value = value.astype(coef.dtype)
        result = jnp.dot(coef[t], value, preferred_element_type=jnp.float32)
        return result, jnp.where(found < tiles, tile_target[0, t], -1)

    def merge(step, carry):
        result, target = moved(step)
        for i in range(blocks):
            s_vmem[i] = s_vmem[i] + jnp.where(target == i, result, 0.0)
        return carry

    late = max(groups // 4, 1)

    def serve(step, carry):
        arrived(step, carry)
        return merge(step, carry)

    with jax.named_scope("arrive"):
        lax.fori_loop(1, groups - late, arrived, 0)
    with jax.named_scope("merge"):
        lax.fori_loop(1, groups - late, merge, 0)
    with jax.named_scope("serve"):
        lax.fori_loop(max(groups - late, 1), groups - 1, serve, 0)
    with jax.named_scope("last"):
        arrived(groups - 1, 0)
    with jax.named_scope("lastmv"):
        result, target = moved(groups - 1)
        outs = []
        for i in range(blocks):
            pre[i] = (s_vmem[i] + jnp.where(target == i, result, 0.0)).astype(pre.dtype)
            outs.append(pltpu.make_async_copy(pre.at[i], pre_out.at[i], out_sem.at[i]))
            if i > 0:
                outs[i - 1].start()
        outs[-1].start()

    def finish(step, carry):
        boundary(step).wait_send()
        keep(step).wait()
        for e in range(1, shards):
            forward(step, e).wait_send()
            keep_far(step, e).wait()
        return carry

    with jax.named_scope("finish"):
        lax.fori_loop(1, groups, finish, 0)
        w_copy.wait()
        for copy in outs:
            copy.wait()


def tile_kernel(
    tile_source,
    tile_target,
    tile_relation,
    coef_hbm,
    pre_hbm,
    received,
    w_hbm,
    out_hbm,
    coef,
    x_tiles,
    w_vmem,
    total,
    pre,
    result,
    seen,
    sems,
):
    tiles = tile_source.shape[1]
    shards, groups = received.shape[:2]
    own = result.shape[0]
    ins = [pltpu.make_async_copy(pre_hbm.at[i], pre.at[i], sems.at[i]) for i in range(own)]
    outs = [
        pltpu.make_async_copy(result.at[i], out_hbm.at[i], sems.at[own + i]) for i in range(own)
    ]
    for copy in ins:
        copy.start()
    for s in range(groups):
        seen[s] = 0

    def look(t, count):
        source = tile_source[0, t] - own

        def repeated():
            before = seen[source]
            seen[source] = 1
            return count + before

        return lax.cond(source >= 0, repeated, lambda: count)

    count = lax.fori_loop(0, tiles, look, 0)

    @pl.when(count == 0)
    def _():
        for i in range(own):
            ins[i].wait()
            result[i] = jnp.maximum(pre[i].astype(jnp.float32), 0.0).astype(result.dtype)
            if i > 0:
                outs[i - 1].start()

    @pl.when(count > 0)
    def _():
        for i in range(own):
            ins[i].wait()
            total[i] = pre[i].astype(jnp.float32)
        for s in range(groups):
            seen[s] = 0

        def add(t, carry):
            source = tile_source[0, t] - own

            @pl.when(source >= 0)
            def _():
                before = seen[source]
                seen[source] = 1

                @pl.when(before == 1)
                def _():
                    copies = [
                        pltpu.make_async_copy(received.at[:, source], x_tiles, sems.at[2 * own]),
                        pltpu.make_async_copy(
                            w_hbm.at[:, tile_relation[0, t]], w_vmem, sems.at[2 * own + 1]
                        ),
                        pltpu.make_async_copy(coef_hbm.at[t], coef, sems.at[2 * own + 2]),
                    ]
                    for copy in copies:
                        copy.start()
                    for copy in copies:
                        copy.wait()
                    value = jnp.dot(x_tiles[0], w_vmem[0], preferred_element_type=jnp.float32)
                    for e in range(1, shards):
                        value = value + jnp.dot(
                            x_tiles[e], w_vmem[e], preferred_element_type=jnp.float32
                        )
                    total[tile_target[0, t]] += jnp.dot(
                        coef[...], value.astype(coef.dtype), preferred_element_type=jnp.float32
                    )

            return carry

        lax.fori_loop(0, tiles, add, 0)
        for i in range(own):
            result[i] = jnp.maximum(total[i], 0.0).astype(result.dtype)
            if i > 0:
                outs[i - 1].start()

    outs[-1].start()
    for copy in outs:
        copy.wait()


def per_device(
    groups,
    shards,
    features,
    rel_weight,
    self_weight,
    type_bias,
    node_type,
    tile_coef,
    tile_source,
    tile_target,
    tile_relation,
    send_block,
    send_live,
):
    rows, width = features.shape
    tiles, block, _ = tile_coef.shape
    relations = rel_weight.shape[0]
    kind = features.dtype
    smem = pl.BlockSpec(memory_space=pltpu.SMEM)
    vmem = pl.BlockSpec(memory_space=pltpu.VMEM)
    anywhere = pl.BlockSpec(memory_space=pl.ANY)
    dma = pltpu.SemaphoreType.DMA
    blocks = rows // block
    lanes = 128 * pl.cdiv(max(tiles, groups, blocks), 128)
    received, weights, pre = pl.pallas_call(
        functools.partial(exchange_kernel, groups, shards, block),
        out_shape=(
            jax.ShapeDtypeStruct((shards, groups, block, width), kind),
            jax.ShapeDtypeStruct((shards, relations, width, width), kind),
            jax.ShapeDtypeStruct((blocks, block, width), kind),
        ),
        in_specs=[smem] * 5 + [vmem] * 4 + [anywhere] * 4,
        out_specs=(anywhere,) * 3,
        scratch_shapes=[
            pltpu.VMEM((groups, block, width), kind),
            pltpu.VMEM((blocks, block, width), kind),
            pltpu.VMEM((shards, blocks, block, width), kind),
            pltpu.VMEM((shards, relations + 1, width, width), kind),
            pltpu.VMEM((blocks, block, width), jnp.float32),
            pltpu.VMEM((tiles, block, block), kind),
            pltpu.VMEM((tiles, block, width), jnp.float32),
            pltpu.VMEM((groups, block, width), kind),
            pltpu.VMEM((shards, groups, block, width), kind),
            pltpu.VMEM((blocks, block, width), kind),
            pltpu.VMEM((8, lanes), jnp.int32),
            pltpu.SMEM((8, lanes), jnp.int32),
            dma((groups,)),
            dma((groups,)),
            dma((max(shards - 1, 1), groups)),
            dma((max(shards - 1, 1), groups)),
            dma((max(shards - 1, 1), 3)),
            dma((max(shards - 1, 1), 3)),
            dma((6,)),
            dma((groups,)),
            dma((max(shards - 1, 1), groups)),
            dma((blocks,)),
        ],
        compiler_params=pltpu.CompilerParams(
            collective_id=0, has_side_effects=True, vmem_limit_bytes=VMEM
        ),
        name="exchange",
    )(
        send_block,
        send_live,
        tile_source,
        tile_target,
        tile_relation,
        tile_source,
        tile_target,
        type_bias,
        node_type.reshape(blocks, block),
        features.reshape(blocks, block, width),
        rel_weight,
        self_weight,
        tile_coef,
    )
    updated = pl.pallas_call(
        tile_kernel,
        out_shape=jax.ShapeDtypeStruct((blocks, block, width), kind),
        in_specs=[smem] * 3 + [anywhere] * 4,
        out_specs=anywhere,
        scratch_shapes=[
            pltpu.VMEM((block, block), kind),
            pltpu.VMEM((shards, block, width), kind),
            pltpu.VMEM((shards, width, width), kind),
            pltpu.VMEM((blocks, block, width), jnp.float32),
            pltpu.VMEM((blocks, block, width), kind),
            pltpu.VMEM((blocks, block, width), kind),
            pltpu.SMEM((groups,), jnp.int32),
            dma((2 * blocks + 3,)),
        ],
        compiler_params=pltpu.CompilerParams(vmem_limit_bytes=VMEM),
        name="tiles",
    )(tile_source, tile_target, tile_relation, tile_coef, pre, received, weights)
    return updated.reshape(rows, width)


def solution(mesh):
    placed = (
        P("graph", "feat"),
        P(None, "feat", None),
        P("feat", None),
        P(None, "feat"),
        P("graph"),
        P("graph", None, None),
        P("graph", None),
        P("graph", None),
        P("graph", None),
        P("graph", None),
        P("graph", None),
    )
    groups, shards = mesh.shape["graph"], mesh.shape["feat"]
    return jax.shard_map(
        functools.partial(per_device, groups, shards),
        mesh=mesh,
        in_specs=placed,
        out_specs=P("graph", "feat"),
        check_vma=False,
    )
```

```python
import functools

import jax
import jax.numpy as jnp
from jax import lax
from jax.experimental import pallas as pl
from jax.experimental.pallas import tpu as pltpu
from jax.sharding import PartitionSpec as P

MESH = pl.DeviceIdType.MESH
VMEM = 67_043_328


def partner(me, step, count):
    other, bit = 0, 1
    while bit < count:
        other = other + ((me // bit + step // bit) % 2) * bit
        bit *= 2
    return other


def exchange_kernel(
    groups,
    shards,
    block,
    send_block_hbm,
    send_live_hbm,
    source_hbm,
    target_hbm,
    relation_hbm,
    bias_hbm,
    type_hbm,
    x_hbm,
    rel_ref,
    self_ref,
    coef_hbm,
    received,
    w_out,
    pre_out,
    outgoing,
    x_own,
    x_far,
    w_all,
    s_vmem,
    coef,
    sums,
    landed,
    far,
    pre,
    plan_vmem,
    plan,
    send_block,
    send_live,
    tile_source,
    tile_target,
    tile_relation,
    source_row,
    target_row,
    bias_ref,
    type_ref,
    small_sem,
    send_sem,
    recv_sem,
    pass_send,
    pass_recv,
    side_send,
    side_recv,
    local_sem,
    keep_sem,
    far_sem,
    out_sem,
):
    me, mine = lax.axis_index("graph"), lax.axis_index("feat")
    blocks, _, width = x_own.shape
    relations = rel_ref.shape[0]
    tiles = coef.shape[0]

    def columns(shard):
        return pl.ds(pl.multiple_of(shard * width, width), width)

    barrier = pltpu.get_barrier_semaphore()

    def greet(step, carry):
        pl.semaphore_signal(
            barrier, inc=1, device_id=(partner(me, step, groups), mine), device_id_type=MESH
        )
        return carry

    lax.fori_loop(1, groups, greet, 0)
    for e in range(1, shards):
        pl.semaphore_signal(
            barrier, inc=1, device_id=(me, (mine + e) % shards), device_id_type=MESH
        )

    x_copy = pltpu.make_async_copy(x_hbm, x_own, local_sem.at[3])
    own_rel = pltpu.make_async_copy(
        rel_ref.at[:, :, columns(mine)], w_all.at[mine, pl.ds(0, relations)], local_sem.at[0]
    )
    own_self = pltpu.make_async_copy(
        self_ref.at[:, columns(mine)], w_all.at[mine, relations], local_sem.at[1]
    )
    coef_copy = pltpu.make_async_copy(coef_hbm, coef, local_sem.at[4])
    smalls = [
        pltpu.make_async_copy(src, dst, small_sem.at[i])
        for i, (src, dst) in enumerate(
            (
                (send_block_hbm, send_block),
                (send_live_hbm, send_live),
                (source_hbm, source_row),
                (target_hbm, target_row),
                (source_hbm, tile_source),
                (target_hbm, tile_target),
                (relation_hbm, tile_relation),
                (bias_hbm, bias_ref),
                (type_hbm, type_ref),
            )
        )
    ]
    x_copy.start()
    for copy in smalls:
        copy.start()
    smalls[0].wait()
    smalls[1].wait()
    x_copy.wait()
    own_rel.start()
    own_self.start()
    coef_copy.start()

    with jax.named_scope("barrier"):
        pl.semaphore_wait(barrier, groups - 1 + shards - 1)

    def boundary(step):
        other = partner(me, step, groups)
        return pltpu.make_async_remote_copy(
            src_ref=outgoing.at[other],
            dst_ref=landed.at[me],
            send_sem=send_sem.at[step],
            recv_sem=recv_sem.at[step],
            device_id=(other, mine),
            device_id_type=MESH,
        )

    half = groups // 2
    inner = (me // half + me // max(half // 2, 1)) % 2

    def turn(i):
        return 1 + (i + inner * (half - 1)) % (groups - 1)

    def gather(i):
        q = partner(me, turn(i), groups)
        picked = x_own[send_block[0, q]].astype(jnp.float32)
        outgoing[q] = (picked * send_live[0, q].astype(jnp.float32)).astype(outgoing.dtype)

    def send(i, carry):
        gather(i + 1)
        boundary(turn(i)).start()
        return carry

    gather(0)
    lax.fori_loop(0, groups - 2, send, 0)
    boundary(turn(groups - 2)).start()

    def side(e):
        peer = (mine + e) % shards
        pairs = (
            (x_own, x_far.at[mine]),
            (self_ref.at[:, columns(peer)], w_all.at[mine, relations]),
            (rel_ref.at[:, :, columns(peer)], w_all.at[mine, pl.ds(0, relations)]),
        )
        return [
            pltpu.make_async_remote_copy(
                src_ref=src,
                dst_ref=dst,
                send_sem=side_send.at[e - 1, i],
                recv_sem=side_recv.at[e - 1, i],
                device_id=(me, peer),
                device_id_type=MESH,
            )
            for i, (src, dst) in enumerate(pairs)
        ]

    sides = [copy for e in range(1, shards) for copy in side(e)]
    for copy in sides:
        copy.start()
    for copy in smalls[2:]:
        copy.wait()

    def iota(shape, axis):
        return lax.broadcasted_iota(jnp.int32, shape, axis)

    square = (tiles, tiles)
    down, along = iota(square, 0), iota(square, 1)

    def column(row):
        return jnp.sum(
            jnp.where(down == along, jnp.broadcast_to(row, square), 0), axis=1, keepdims=True
        )

    sources = column(source_row[...])
    keys_row = jnp.where(source_row[...] < blocks, target_row[...], blocks)
    keys = column(keys_row)
    ahead = (keys_row < keys) | ((keys_row == keys) & (along < down))
    rank = jnp.sum(ahead.astype(jnp.int32), axis=1, keepdims=True)
    plan_vmem[0:1, 0:tiles] = jnp.sum(
        jnp.where(rank == along, down, 0), axis=0, keepdims=True
    )
    wide = (tiles, groups)
    plan_vmem[1:2, 0:groups] = jnp.min(
        jnp.where(sources == blocks + iota(wide, 1), iota(wide, 0), tiles), axis=0, keepdims=True
    )
    each = (tiles, blocks)
    plan_vmem[2:3, 0:blocks] = jnp.sum(
        (keys <= iota(each, 1)).astype(jnp.int32), axis=0, keepdims=True
    )
    plan_vmem[3:4, 0:blocks] = jnp.sum(
        (keys == iota(each, 1)).astype(jnp.int32), axis=0, keepdims=True
    )
    plan_copy = pltpu.make_async_copy(plan_vmem, plan, local_sem.at[5])
    plan_copy.start()
    own_rel.wait()
    own_self.wait()
    with jax.named_scope("sides"):
        for copy in sides:
            copy.wait()
    w_copy = pltpu.make_async_copy(
        w_all.at[:, pl.ds(0, relations)], w_out, local_sem.at[2]
    )
    w_copy.start()

    chunk = 2

    def full_dot(start, relation):
        at = pl.ds(start, chunk)
        total = jnp.dot(
            x_own[at].reshape(chunk * block, width),
            w_all[mine, relation],
            preferred_element_type=jnp.float32,
        )
        for e in range(1, shards):
            peer = (mine + e) % shards
            total = total + jnp.dot(
                x_far[peer, at].reshape(chunk * block, width),
                w_all[peer, relation],
                preferred_element_type=jnp.float32,
            )
        return total.reshape(chunk, block, width)

    def own_part(i, carry):
        s_vmem[pl.ds(i * chunk, chunk)] = full_dot(i * chunk, relations)
        return carry

    with jax.named_scope("self"):
        lax.fori_loop(0, blocks // chunk, own_part, 0)

    coef_copy.wait()
    plan_copy.wait()
    stride = 4 if tiles % 4 == 0 else 1

    def local(i, carry):
        terms = []
        for j in range(stride):
            t = plan[0, i * stride + j]
            relation = tile_relation[0, t]
            source = jnp.minimum(tile_source[0, t], blocks - 1)
            value = jnp.dot(
                x_own[source], w_all[mine, relation], preferred_element_type=jnp.float32
            )
            for e in range(1, shards):
                peer = (mine + e) % shards
                value = value + jnp.dot(
                    x_far[peer, source], w_all[peer, relation], preferred_element_type=jnp.float32
                )
            terms.append((t, value.astype(coef.dtype)))
        for j, (t, value) in enumerate(terms):
            at = i * stride + j
            before = plan[0, jnp.maximum(at - 1, 0)]
            joins = (tile_target[0, t] == tile_target[0, before]) & (at > 0)
            term = jnp.dot(coef[t], value, preferred_element_type=jnp.float32)
            sums[at] = term + jnp.where(joins, sums[jnp.maximum(at - 1, 0)], 0.0)
        return carry

    with jax.named_scope("local"):
        lax.fori_loop(0, tiles // stride, local, 0)

    with jax.named_scope("base"):
        for i in range(blocks):
            kinds = jnp.transpose(jnp.broadcast_to(type_ref[i : i + 1, :], (block, block)))
            kinds = jnp.concatenate([kinds] * (width // block), axis=1)
            total = s_vmem[i]
            for kind in range(bias_ref.shape[0]):
                total = total + jnp.where(kinds == kind, bias_ref[kind : kind + 1, :], 0.0)
            last = jnp.maximum(plan[2, i] - 1, 0)
            s_vmem[i] = total + jnp.where(plan[3, i] > 0, sums[last], 0.0)

    def forward(step, e):
        other = partner(me, step, groups)
        return pltpu.make_async_remote_copy(
            src_ref=landed.at[other],
            dst_ref=far.at[mine, other],
            send_sem=pass_send.at[e - 1, step],
            recv_sem=pass_recv.at[e - 1, step],
            device_id=(me, (mine + e) % shards),
            device_id_type=MESH,
        )

    def keep(step):
        other = partner(me, step, groups)
        return pltpu.make_async_copy(
            landed.at[other], received.at[mine, other], keep_sem.at[step]
        )

    def keep_far(step, e):
        origin, other = (mine + shards - e) % shards, partner(me, step, groups)
        return pltpu.make_async_copy(
            far.at[origin, other], received.at[origin, other], far_sem.at[e - 1, step]
        )

    def arrived(step, carry):
        boundary(step).wait_recv()
        for e in range(1, shards):
            forward(step, e).start()
        keep(step).start()
        return carry

    def moved(step):
        other = partner(me, step, groups)
        found = plan[1, other]
        t = jnp.minimum(found, tiles - 1)
        relation = tile_relation[0, t]
        value = jnp.dot(
            landed[other], w_all[mine, relation], preferred_element_type=jnp.float32
        )
        for e in range(1, shards):
            origin = (mine + shards - e) % shards
            pltpu.make_async_remote_copy(
                src_ref=far.at[origin, other],
                dst_ref=far.at[origin, other],
                send_sem=pass_send.at[e - 1, step],
                recv_sem=pass_recv.at[e - 1, step],
                device_id=(me, (mine + e) % shards),
                device_id_type=MESH,
            ).wait_recv()
            keep_far(step, e).start()
            value = value + jnp.dot(
                far[origin, other], w_all[origin, relation], preferred_element_type=jnp.float32
            )
        value = value.astype(coef.dtype)
        result = jnp.dot(coef[t], value, preferred_element_type=jnp.float32)
        return result, jnp.where(found < tiles, tile_target[0, t], -1)

    def merge(step, carry):
        result, target = moved(step)
        for i in range(blocks):
            s_vmem[i] = s_vmem[i] + jnp.where(target == i, result, 0.0)
        return carry

    ready = max(3 * groups // 4, 1)

    def serve(step, carry):
        arrived(step, carry)
        return merge(step - 1, carry)

    with jax.named_scope("arrive"):
        lax.fori_loop(1, ready, arrived, 0)
    with jax.named_scope("merge"):
        lax.fori_loop(1, ready - 1, merge, 0)
    with jax.named_scope("serve"):
        lax.fori_loop(ready, groups - 1, serve, 0)
    with jax.named_scope("last"):
        arrived(groups - 1, 0)
        merge(groups - 2, 0)
    with jax.named_scope("lastmv"):
        result, target = moved(groups - 1)
        outs = []
        for i in range(blocks):
            pre[i] = (s_vmem[i] + jnp.where(target == i, result, 0.0)).astype(pre.dtype)
            outs.append(pltpu.make_async_copy(pre.at[i], pre_out.at[i], out_sem.at[i]))
            if i > 0:
                outs[i - 1].start()
        outs[-1].start()

    def finish(step, carry):
        boundary(step).wait_send()
        keep(step).wait()
        for e in range(1, shards):
            forward(step, e).wait_send()
            keep_far(step, e).wait()
        return carry

    with jax.named_scope("finish"):
        lax.fori_loop(1, groups, finish, 0)
        w_copy.wait()
        for copy in outs:
            copy.wait()


def tile_kernel(
    tile_source,
    tile_target,
    tile_relation,
    coef_hbm,
    pre_hbm,
    received,
    w_hbm,
    out_hbm,
    coef,
    x_tiles,
    w_vmem,
    total,
    pre,
    result,
    seen,
    sems,
):
    tiles = tile_source.shape[1]
    shards, groups = received.shape[:2]
    own = result.shape[0]
    ins = [pltpu.make_async_copy(pre_hbm.at[i], pre.at[i], sems.at[i]) for i in range(own)]
    outs = [
        pltpu.make_async_copy(result.at[i], out_hbm.at[i], sems.at[own + i]) for i in range(own)
    ]
    for copy in ins:
        copy.start()
    for s in range(groups):
        seen[s] = 0

    def look(t, count):
        source = tile_source[0, t] - own

        def repeated():
            before = seen[source]
            seen[source] = 1
            return count + before

        return lax.cond(source >= 0, repeated, lambda: count)

    count = lax.fori_loop(0, tiles, look, 0)

    @pl.when(count == 0)
    def _():
        for i in range(own):
            ins[i].wait()
            result[i] = jnp.maximum(pre[i].astype(jnp.float32), 0.0).astype(result.dtype)
            if i > 0:
                outs[i - 1].start()

    @pl.when(count > 0)
    def _():
        for i in range(own):
            ins[i].wait()
            total[i] = pre[i].astype(jnp.float32)
        for s in range(groups):
            seen[s] = 0

        def add(t, carry):
            source = tile_source[0, t] - own

            @pl.when(source >= 0)
            def _():
                before = seen[source]
                seen[source] = 1

                @pl.when(before == 1)
                def _():
                    copies = [
                        pltpu.make_async_copy(received.at[:, source], x_tiles, sems.at[2 * own]),
                        pltpu.make_async_copy(
                            w_hbm.at[:, tile_relation[0, t]], w_vmem, sems.at[2 * own + 1]
                        ),
                        pltpu.make_async_copy(coef_hbm.at[t], coef, sems.at[2 * own + 2]),
                    ]
                    for copy in copies:
                        copy.start()
                    for copy in copies:
                        copy.wait()
                    value = jnp.dot(x_tiles[0], w_vmem[0], preferred_element_type=jnp.float32)
                    for e in range(1, shards):
                        value = value + jnp.dot(
                            x_tiles[e], w_vmem[e], preferred_element_type=jnp.float32
                        )
                    total[tile_target[0, t]] += jnp.dot(
                        coef[...], value.astype(coef.dtype), preferred_element_type=jnp.float32
                    )

            return carry

        lax.fori_loop(0, tiles, add, 0)
        for i in range(own):
            result[i] = jnp.maximum(total[i], 0.0).astype(result.dtype)
            if i > 0:
                outs[i - 1].start()

    outs[-1].start()
    for copy in outs:
        copy.wait()


def per_device(
    groups,
    shards,
    features,
    rel_weight,
    self_weight,
    type_bias,
    node_type,
    tile_coef,
    tile_source,
    tile_target,
    tile_relation,
    send_block,
    send_live,
):
    rows, width = features.shape
    tiles, block, _ = tile_coef.shape
    relations = rel_weight.shape[0]
    kind = features.dtype
    smem = pl.BlockSpec(memory_space=pltpu.SMEM)
    vmem = pl.BlockSpec(memory_space=pltpu.VMEM)
    anywhere = pl.BlockSpec(memory_space=pl.ANY)
    dma = pltpu.SemaphoreType.DMA
    blocks = rows // block
    lanes = 128 * pl.cdiv(max(tiles, groups, blocks), 128)
    received, weights, pre = pl.pallas_call(
        functools.partial(exchange_kernel, groups, shards, block),
        out_shape=(
            jax.ShapeDtypeStruct((shards, groups, block, width), kind),
            jax.ShapeDtypeStruct((shards, relations, width, width), kind),
            jax.ShapeDtypeStruct((blocks, block, width), kind),
        ),
        in_specs=[anywhere] * 11,
        out_specs=(anywhere,) * 3,
        scratch_shapes=[
            pltpu.VMEM((groups, block, width), kind),
            pltpu.VMEM((blocks, block, width), kind),
            pltpu.VMEM((shards, blocks, block, width), kind),
            pltpu.VMEM((shards, relations + 1, width, width), kind),
            pltpu.VMEM((blocks, block, width), jnp.float32),
            pltpu.VMEM((tiles, block, block), kind),
            pltpu.VMEM((tiles, block, width), jnp.float32),
            pltpu.VMEM((groups, block, width), kind),
            pltpu.VMEM((shards, groups, block, width), kind),
            pltpu.VMEM((blocks, block, width), kind),
            pltpu.VMEM((8, lanes), jnp.int32),
            pltpu.SMEM((8, lanes), jnp.int32),
            pltpu.SMEM(send_block.shape, jnp.int32),
            pltpu.SMEM(send_block.shape, jnp.int32),
            pltpu.SMEM(tile_source.shape, jnp.int32),
            pltpu.SMEM(tile_source.shape, jnp.int32),
            pltpu.SMEM(tile_source.shape, jnp.int32),
            pltpu.VMEM(tile_source.shape, jnp.int32),
            pltpu.VMEM(tile_source.shape, jnp.int32),
            pltpu.VMEM(type_bias.shape, jnp.float32),
            pltpu.VMEM((blocks, block), jnp.int32),
            dma((9,)),
            dma((groups,)),
            dma((groups,)),
            dma((max(shards - 1, 1), groups)),
            dma((max(shards - 1, 1), groups)),
            dma((max(shards - 1, 1), 3)),
            dma((max(shards - 1, 1), 3)),
            dma((6,)),
            dma((groups,)),
            dma((max(shards - 1, 1), groups)),
            dma((blocks,)),
        ],
        compiler_params=pltpu.CompilerParams(
            collective_id=0, has_side_effects=True, vmem_limit_bytes=VMEM
        ),
        name="exchange",
    )(
        send_block,
        send_live,
        tile_source,
        tile_target,
        tile_relation,
        type_bias,
        node_type.reshape(blocks, block),
        features.reshape(blocks, block, width),
        rel_weight,
        self_weight,
        tile_coef,
    )
    updated = pl.pallas_call(
        tile_kernel,
        out_shape=jax.ShapeDtypeStruct((blocks, block, width), kind),
        in_specs=[smem] * 3 + [anywhere] * 4,
        out_specs=anywhere,
        scratch_shapes=[
            pltpu.VMEM((block, block), kind),
            pltpu.VMEM((shards, block, width), kind),
            pltpu.VMEM((shards, width, width), kind),
            pltpu.VMEM((blocks, block, width), jnp.float32),
            pltpu.VMEM((blocks, block, width), kind),
            pltpu.VMEM((blocks, block, width), kind),
            pltpu.SMEM((groups,), jnp.int32),
            dma((2 * blocks + 3,)),
        ],
        compiler_params=pltpu.CompilerParams(vmem_limit_bytes=VMEM),
        name="tiles",
    )(tile_source, tile_target, tile_relation, tile_coef, pre, received, weights)
    return updated.reshape(rows, width)


def solution(mesh):
    placed = (
        P("graph", "feat"),
        P(None, "feat", None),
        P("feat", None),
        P(None, "feat"),
        P("graph"),
        P("graph", None, None),
        P("graph", None),
        P("graph", None),
        P("graph", None),
        P("graph", None),
        P("graph", None),
    )
    groups, shards = mesh.shape["graph"], mesh.shape["feat"]
    return jax.shard_map(
        functools.partial(per_device, groups, shards),
        mesh=mesh,
        in_specs=placed,
        out_specs=P("graph", "feat"),
        check_vma=False,
    )
```

```python
import functools

import jax
import jax.numpy as jnp
from jax import lax
from jax.experimental import pallas as pl
from jax.experimental.pallas import tpu as pltpu
from jax.sharding import PartitionSpec as P

MESH = pl.DeviceIdType.MESH
VMEM = 67_043_328


def partner(me, step, count):
    other, bit = 0, 1
    while bit < count:
        other = other + ((me // bit + step // bit) % 2) * bit
        bit *= 2
    return other


def exchange_kernel(
    groups,
    shards,
    block,
    send_block_hbm,
    send_live_hbm,
    source_hbm,
    target_hbm,
    relation_hbm,
    bias_hbm,
    type_hbm,
    x_hbm,
    rel_ref,
    self_ref,
    coef_hbm,
    received,
    w_out,
    pre_out,
    outgoing,
    x_own,
    x_far,
    w_all,
    s_vmem,
    coef,
    sums,
    landed,
    far,
    pre,
    plan_vmem,
    plan,
    send_block,
    send_live,
    tile_source,
    tile_target,
    tile_relation,
    source_row,
    target_row,
    bias_ref,
    type_ref,
    small_sem,
    send_sem,
    recv_sem,
    pass_send,
    pass_recv,
    side_send,
    side_recv,
    local_sem,
    keep_sem,
    far_sem,
    out_sem,
):
    me, mine = lax.axis_index("graph"), lax.axis_index("feat")
    blocks, _, width = x_own.shape
    relations = rel_ref.shape[0]
    tiles = coef.shape[0]

    def columns(shard):
        return pl.ds(pl.multiple_of(shard * width, width), width)

    barrier = pltpu.get_barrier_semaphore()

    def greet(step, carry):
        pl.semaphore_signal(
            barrier, inc=1, device_id=(partner(me, step, groups), mine), device_id_type=MESH
        )
        return carry

    lax.fori_loop(1, groups, greet, 0)
    for e in range(1, shards):
        pl.semaphore_signal(
            barrier, inc=1, device_id=(me, (mine + e) % shards), device_id_type=MESH
        )

    x_copy = pltpu.make_async_copy(x_hbm, x_own, local_sem.at[3])
    own_rel = pltpu.make_async_copy(
        rel_ref.at[:, :, columns(mine)], w_all.at[mine, pl.ds(0, relations)], local_sem.at[0]
    )
    own_self = pltpu.make_async_copy(
        self_ref.at[:, columns(mine)], w_all.at[mine, relations], local_sem.at[1]
    )
    coef_copy = pltpu.make_async_copy(coef_hbm, coef, local_sem.at[4])
    smalls = [
        pltpu.make_async_copy(src, dst, small_sem.at[i])
        for i, (src, dst) in enumerate(
            (
                (send_block_hbm, send_block),
                (send_live_hbm, send_live),
                (source_hbm, source_row),
                (target_hbm, target_row),
                (source_hbm, tile_source),
                (target_hbm, tile_target),
                (relation_hbm, tile_relation),
                (bias_hbm, bias_ref),
                (type_hbm, type_ref),
            )
        )
    ]
    x_copy.start()
    for copy in smalls:
        copy.start()
    smalls[0].wait()
    smalls[1].wait()
    x_copy.wait()
    own_rel.start()
    own_self.start()
    coef_copy.start()

    with jax.named_scope("barrier"):
        pl.semaphore_wait(barrier, groups - 1 + shards - 1)

    def boundary(step):
        other = partner(me, step, groups)
        return pltpu.make_async_remote_copy(
            src_ref=outgoing.at[other],
            dst_ref=landed.at[me],
            send_sem=send_sem.at[step],
            recv_sem=recv_sem.at[step],
            device_id=(other, mine),
            device_id_type=MESH,
        )

    half = groups // 2
    inner = (me // half + me // max(half // 2, 1)) % 2

    def turn(i):
        return 1 + (i + inner * (half - 1)) % (groups - 1)

    def gather(i):
        q = partner(me, turn(i), groups)
        picked = x_own[send_block[0, q]].astype(jnp.float32)
        outgoing[q] = (picked * send_live[0, q].astype(jnp.float32)).astype(outgoing.dtype)

    def send(i, carry):
        gather(i + 1)
        boundary(turn(i)).start()
        return carry

    gather(0)
    lax.fori_loop(0, groups - 2, send, 0)
    boundary(turn(groups - 2)).start()

    def side(e):
        peer = (mine + e) % shards
        pairs = (
            (x_own, x_far.at[mine]),
            (self_ref.at[:, columns(peer)], w_all.at[mine, relations]),
            (rel_ref.at[:, :, columns(peer)], w_all.at[mine, pl.ds(0, relations)]),
        )
        return [
            pltpu.make_async_remote_copy(
                src_ref=src,
                dst_ref=dst,
                send_sem=side_send.at[e - 1, i],
                recv_sem=side_recv.at[e - 1, i],
                device_id=(me, peer),
                device_id_type=MESH,
            )
            for i, (src, dst) in enumerate(pairs)
        ]

    sides = [copy for e in range(1, shards) for copy in side(e)]
    for copy in sides:
        copy.start()
    for copy in smalls[2:]:
        copy.wait()

    def iota(shape, axis):
        return lax.broadcasted_iota(jnp.int32, shape, axis)

    square = (tiles, tiles)
    down, along = iota(square, 0), iota(square, 1)

    def column(row):
        return jnp.sum(
            jnp.where(down == along, jnp.broadcast_to(row, square), 0), axis=1, keepdims=True
        )

    sources = column(source_row[...])
    keys_row = jnp.where(source_row[...] < blocks, target_row[...], blocks)
    keys = column(keys_row)
    ahead = (keys_row < keys) | ((keys_row == keys) & (along < down))
    rank = jnp.sum(ahead.astype(jnp.int32), axis=1, keepdims=True)
    plan_vmem[0:1, 0:tiles] = jnp.sum(
        jnp.where(rank == along, down, 0), axis=0, keepdims=True
    )
    wide = (tiles, groups)
    plan_vmem[1:2, 0:groups] = jnp.min(
        jnp.where(sources == blocks + iota(wide, 1), iota(wide, 0), tiles), axis=0, keepdims=True
    )
    each = (tiles, blocks)
    plan_vmem[2:3, 0:blocks] = jnp.sum(
        (keys <= iota(each, 1)).astype(jnp.int32), axis=0, keepdims=True
    )
    plan_vmem[3:4, 0:blocks] = jnp.sum(
        (keys == iota(each, 1)).astype(jnp.int32), axis=0, keepdims=True
    )
    plan_copy = pltpu.make_async_copy(plan_vmem, plan, local_sem.at[5])
    plan_copy.start()
    own_rel.wait()
    own_self.wait()
    with jax.named_scope("sides"):
        for copy in sides:
            copy.wait()
    w_copy = pltpu.make_async_copy(
        w_all.at[:, pl.ds(0, relations)], w_out, local_sem.at[2]
    )
    w_copy.start()

    chunk = 2

    def full_dot(start, relation):
        at = pl.ds(start, chunk)
        total = jnp.dot(
            x_own[at].reshape(chunk * block, width),
            w_all[mine, relation],
            preferred_element_type=jnp.float32,
        )
        for e in range(1, shards):
            peer = (mine + e) % shards
            total = total + jnp.dot(
                x_far[peer, at].reshape(chunk * block, width),
                w_all[peer, relation],
                preferred_element_type=jnp.float32,
            )
        return total.reshape(chunk, block, width)

    def own_part(i, carry):
        s_vmem[pl.ds(i * chunk, chunk)] = full_dot(i * chunk, relations)
        return carry

    with jax.named_scope("self"):
        lax.fori_loop(0, blocks // chunk, own_part, 0)

    coef_copy.wait()
    plan_copy.wait()
    stride = 4 if tiles % 4 == 0 else 1

    def local(i, carry):
        terms = []
        for j in range(stride):
            t = plan[0, i * stride + j]
            relation = tile_relation[0, t]
            source = jnp.minimum(tile_source[0, t], blocks - 1)
            value = jnp.dot(
                x_own[source], w_all[mine, relation], preferred_element_type=jnp.float32
            )
            for e in range(1, shards):
                peer = (mine + e) % shards
                value = value + jnp.dot(
                    x_far[peer, source], w_all[peer, relation], preferred_element_type=jnp.float32
                )
            terms.append((t, value.astype(coef.dtype)))
        for j, (t, value) in enumerate(terms):
            at = i * stride + j
            before = plan[0, jnp.maximum(at - 1, 0)]
            joins = (tile_target[0, t] == tile_target[0, before]) & (at > 0)
            term = jnp.dot(coef[t], value, preferred_element_type=jnp.float32)
            sums[at] = term + jnp.where(joins, sums[jnp.maximum(at - 1, 0)], 0.0)
        return carry

    with jax.named_scope("local"):
        lax.fori_loop(0, tiles // stride, local, 0)

    with jax.named_scope("base"):
        for i in range(blocks):
            kinds = jnp.transpose(jnp.broadcast_to(type_ref[i : i + 1, :], (block, block)))
            kinds = jnp.concatenate([kinds] * (width // block), axis=1)
            total = s_vmem[i]
            for kind in range(bias_ref.shape[0]):
                total = total + jnp.where(kinds == kind, bias_ref[kind : kind + 1, :], 0.0)
            last = jnp.maximum(plan[2, i] - 1, 0)
            s_vmem[i] = total + jnp.where(plan[3, i] > 0, sums[last], 0.0)

    def forward(step, e):
        other = partner(me, step, groups)
        return pltpu.make_async_remote_copy(
            src_ref=landed.at[other],
            dst_ref=far.at[mine, other],
            send_sem=pass_send.at[e - 1, step],
            recv_sem=pass_recv.at[e - 1, step],
            device_id=(me, (mine + e) % shards),
            device_id_type=MESH,
        )

    def keep(step):
        other = partner(me, step, groups)
        return pltpu.make_async_copy(
            landed.at[other], received.at[mine, other], keep_sem.at[step]
        )

    def keep_far(step, e):
        origin, other = (mine + shards - e) % shards, partner(me, step, groups)
        return pltpu.make_async_copy(
            far.at[origin, other], received.at[origin, other], far_sem.at[e - 1, step]
        )

    def arrived(step, carry):
        boundary(step).wait_recv()
        for e in range(1, shards):
            forward(step, e).start()
        keep(step).start()
        return carry

    def moved(step):
        other = partner(me, step, groups)
        found = plan[1, other]
        t = jnp.minimum(found, tiles - 1)
        relation = tile_relation[0, t]
        value = jnp.dot(
            landed[other], w_all[mine, relation], preferred_element_type=jnp.float32
        )
        for e in range(1, shards):
            origin = (mine + shards - e) % shards
            pltpu.make_async_remote_copy(
                src_ref=far.at[origin, other],
                dst_ref=far.at[origin, other],
                send_sem=pass_send.at[e - 1, step],
                recv_sem=pass_recv.at[e - 1, step],
                device_id=(me, (mine + e) % shards),
                device_id_type=MESH,
            ).wait_recv()
            keep_far(step, e).start()
            value = value + jnp.dot(
                far[origin, other], w_all[origin, relation], preferred_element_type=jnp.float32
            )
        value = value.astype(coef.dtype)
        result = jnp.dot(coef[t], value, preferred_element_type=jnp.float32)
        return result, jnp.where(found < tiles, tile_target[0, t], -1)

    def merge(step, carry):
        result, target = moved(step)
        for i in range(blocks):
            s_vmem[i] = s_vmem[i] + jnp.where(target == i, result, 0.0)
        return carry

    late = max(groups // 4, 1)

    def serve(step, carry):
        arrived(step, carry)
        return merge(step, carry)

    with jax.named_scope("arrive"):
        lax.fori_loop(1, groups - late, arrived, 0)
    with jax.named_scope("merge"):
        lax.fori_loop(1, groups - late, merge, 0)
    with jax.named_scope("serve"):
        lax.fori_loop(max(groups - late, 1), groups - 1, serve, 0)
    with jax.named_scope("last"):
        arrived(groups - 1, 0)
    with jax.named_scope("lastmv"):
        result, target = moved(groups - 1)
        outs = []
        for i in range(blocks):
            pre[i] = (s_vmem[i] + jnp.where(target == i, result, 0.0)).astype(pre.dtype)
            outs.append(pltpu.make_async_copy(pre.at[i], pre_out.at[i], out_sem.at[i]))
            if i > 0:
                outs[i - 1].start()
        outs[-1].start()

    def finish(step, carry):
        boundary(step).wait_send()
        keep(step).wait()
        for e in range(1, shards):
            forward(step, e).wait_send()
            keep_far(step, e).wait()
        return carry

    with jax.named_scope("finish"):
        lax.fori_loop(1, groups, finish, 0)
        w_copy.wait()
        for copy in outs:
            copy.wait()


def relay_kernel(
    groups,
    shards,
    block,
    send_block_hbm,
    send_live_hbm,
    source_hbm,
    target_hbm,
    relation_hbm,
    bias_hbm,
    type_hbm,
    x_hbm,
    rel_ref,
    self_ref,
    coef_hbm,
    pre_out,
    flag_out,
    outgoing,
    x_own,
    x_far,
    w_all,
    s_vmem,
    coef,
    sums,
    landed,
    far,
    list_out,
    list_in,
    relayed,
    table_out,
    table_in,
    table,
    flags,
    flag_vmem,
    plan_vmem,
    plan,
    send_block,
    send_live,
    tile_source,
    tile_target,
    tile_relation,
    source_row,
    target_row,
    bias_ref,
    type_ref,
    small_sem,
    send_sem,
    recv_sem,
    pass_send,
    pass_recv,
    side_send,
    side_recv,
    local_sem,
    list_send,
    list_recv,
    relay_send,
    flag_send,
    flag_recv,
    table_sem,
):
    me, mine = lax.axis_index("graph"), lax.axis_index("feat")
    blocks, _, width = x_own.shape
    relations = rel_ref.shape[0]
    tiles = coef.shape[0]

    def columns(shard):
        return pl.ds(pl.multiple_of(shard * width, width), width)

    barrier = pltpu.get_barrier_semaphore()

    def greet(step, carry):
        pl.semaphore_signal(
            barrier, inc=1, device_id=(partner(me, step, groups), mine), device_id_type=MESH
        )
        return carry

    lax.fori_loop(1, groups, greet, 0)
    for e in range(1, shards):
        pl.semaphore_signal(
            barrier, inc=1, device_id=(me, (mine + e) % shards), device_id_type=MESH
        )

    x_copy = pltpu.make_async_copy(x_hbm, x_own, local_sem.at[3])
    own_rel = pltpu.make_async_copy(
        rel_ref.at[:, :, columns(mine)], w_all.at[mine, pl.ds(0, relations)], local_sem.at[0]
    )
    own_self = pltpu.make_async_copy(
        self_ref.at[:, columns(mine)], w_all.at[mine, relations], local_sem.at[1]
    )
    coef_copy = pltpu.make_async_copy(coef_hbm, coef, local_sem.at[4])
    smalls = [
        pltpu.make_async_copy(src, dst, small_sem.at[i])
        for i, (src, dst) in enumerate(
            (
                (send_block_hbm, send_block),
                (send_live_hbm, send_live),
                (source_hbm, source_row),
                (target_hbm, target_row),
                (source_hbm, tile_source),
                (target_hbm, tile_target),
                (relation_hbm, tile_relation),
                (bias_hbm, bias_ref),
                (type_hbm, type_ref),
            )
        )
    ]
    x_copy.start()
    for copy in smalls:
        copy.start()
    smalls[0].wait()
    smalls[1].wait()
    x_copy.wait()
    own_rel.start()
    own_self.start()
    coef_copy.start()

    def boundary(step):
        other = partner(me, step, groups)
        return pltpu.make_async_remote_copy(
            src_ref=outgoing.at[other],
            dst_ref=landed.at[me],
            send_sem=send_sem.at[step],
            recv_sem=recv_sem.at[step],
            device_id=(other, mine),
            device_id_type=MESH,
        )

    plane = groups // 4
    level = me // plane
    middle = (level + level // 2) % 2
    inner, outer = middle == 1, middle == 0

    def gather(step, carry):
        q = partner(me, step, groups)
        picked = x_own[send_block[0, q]].astype(jnp.float32)
        outgoing[q] = (picked * send_live[0, q].astype(jnp.float32)).astype(outgoing.dtype)
        return carry

    def send(step, carry):
        boundary(step).start()
        return carry

    lax.fori_loop(1, groups, gather, 0)
    smalls[2].wait()

    def iota(shape, axis):
        return lax.broadcasted_iota(jnp.int32, shape, axis)

    square = (tiles, tiles)
    down, along = iota(square, 0), iota(square, 1)

    def column(row):
        return jnp.sum(
            jnp.where(down == along, jnp.broadcast_to(row, square), 0), axis=1, keepdims=True
        )

    sources = column(source_row[...])
    wide = (tiles, groups)
    first_row = jnp.min(
        jnp.where(sources == blocks + iota(wide, 1), iota(wide, 0), tiles), axis=0, keepdims=True
    )
    plan_vmem[1:2, 0:groups] = first_row
    named = (first_row < tiles).astype(jnp.int32)
    repeats = jnp.sum(
        (source_row[...] >= blocks).astype(jnp.int32), axis=1, keepdims=True
    ) - jnp.sum(named, axis=1, keepdims=True)
    flags[me] = jnp.broadcast_to(repeats, flags.shape[1:])

    def flagged(step):
        return pltpu.make_async_remote_copy(
            src_ref=flags.at[me],
            dst_ref=flags.at[me],
            send_sem=flag_send.at[step],
            recv_sem=flag_recv.at[step],
            device_id=(partner(me, step, groups), mine),
            device_id_type=MESH,
        )

    with jax.named_scope("barrier"):
        pl.semaphore_wait(barrier, groups - 1 + shards - 1)

    def tell(step, carry):
        flagged(step).start()
        return carry

    lax.fori_loop(1, groups, tell, 0)
    @pl.when(inner)
    def _():
        lax.fori_loop(2 * plane, groups, send, 0)

    lax.fori_loop(1, 2 * plane, send, 0)

    @pl.when(outer)
    def _():
        lax.fori_loop(2 * plane, groups, send, 0)

    def side(e):
        peer = (mine + e) % shards
        pairs = (
            (x_own, x_far.at[mine]),
            (self_ref.at[:, columns(peer)], w_all.at[mine, relations]),
            (rel_ref.at[:, :, columns(peer)], w_all.at[mine, pl.ds(0, relations)]),
        )
        return [
            pltpu.make_async_remote_copy(
                src_ref=src,
                dst_ref=dst,
                send_sem=side_send.at[e - 1, i],
                recv_sem=side_recv.at[e - 1, i],
                device_id=(me, peer),
                device_id_type=MESH,
            )
            for i, (src, dst) in enumerate(pairs)
        ]

    sides = [copy for e in range(1, shards) for copy in side(e)]
    for copy in sides:
        copy.start()
    for copy in smalls[3:]:
        copy.wait()

    keys_row = jnp.where(source_row[...] < blocks, target_row[...], blocks)
    keys = column(keys_row)
    ahead = (keys_row < keys) | ((keys_row == keys) & (along < down))
    rank = jnp.sum(ahead.astype(jnp.int32), axis=1, keepdims=True)
    plan_vmem[0:1, 0:tiles] = jnp.sum(
        jnp.where(rank == along, down, 0), axis=0, keepdims=True
    )
    each = (tiles, blocks)
    plan_vmem[2:3, 0:blocks] = jnp.sum(
        (keys <= iota(each, 1)).astype(jnp.int32), axis=0, keepdims=True
    )
    plan_vmem[3:4, 0:blocks] = jnp.sum(
        (keys == iota(each, 1)).astype(jnp.int32), axis=0, keepdims=True
    )
    plan_copy = pltpu.make_async_copy(plan_vmem, plan, local_sem.at[5])
    plan_copy.start()
    own_rel.wait()
    own_self.wait()
    with jax.named_scope("sides"):
        for copy in sides:
            copy.wait()
    chunk = 2

    def full_dot(start, relation):
        at = pl.ds(start, chunk)
        total = jnp.dot(
            x_own[at].reshape(chunk * block, width),
            w_all[mine, relation],
            preferred_element_type=jnp.float32,
        )
        for e in range(1, shards):
            peer = (mine + e) % shards
            total = total + jnp.dot(
                x_far[peer, at].reshape(chunk * block, width),
                w_all[peer, relation],
                preferred_element_type=jnp.float32,
            )
        return total.reshape(chunk, block, width)

    def own_part(i, carry):
        s_vmem[pl.ds(i * chunk, chunk)] = full_dot(i * chunk, relations)
        return carry

    with jax.named_scope("self"):
        lax.fori_loop(0, blocks // chunk, own_part, 0)

    coef_copy.wait()
    plan_copy.wait()
    stride = 4 if tiles % 4 == 0 else 1

    def local(i, carry):
        terms = []
        for j in range(stride):
            t = plan[0, i * stride + j]
            relation = tile_relation[0, t]
            source = jnp.minimum(tile_source[0, t], blocks - 1)
            value = jnp.dot(
                x_own[source], w_all[mine, relation], preferred_element_type=jnp.float32
            )
            for e in range(1, shards):
                peer = (mine + e) % shards
                value = value + jnp.dot(
                    x_far[peer, source], w_all[peer, relation], preferred_element_type=jnp.float32
                )
            terms.append((t, value.astype(coef.dtype)))
        for j, (t, value) in enumerate(terms):
            at = i * stride + j
            before = plan[0, jnp.maximum(at - 1, 0)]
            joins = (tile_target[0, t] == tile_target[0, before]) & (at > 0)
            term = jnp.dot(coef[t], value, preferred_element_type=jnp.float32)
            sums[at] = term + jnp.where(joins, sums[jnp.maximum(at - 1, 0)], 0.0)
        return carry

    ahead_of_relay = 7 * tiles // (10 * stride)
    with jax.named_scope("local"):
        lax.fori_loop(0, ahead_of_relay, local, 0)

    with jax.named_scope("local2"):
        lax.fori_loop(ahead_of_relay, tiles // stride, local, 0)

    with jax.named_scope("base"):
        for i in range(blocks):
            kinds = jnp.transpose(jnp.broadcast_to(type_ref[i : i + 1, :], (block, block)))
            kinds = jnp.concatenate([kinds] * (width // block), axis=1)
            total = s_vmem[i]
            for kind in range(bias_ref.shape[0]):
                total = total + jnp.where(kinds == kind, bias_ref[kind : kind + 1, :], 0.0)
            last = jnp.maximum(plan[2, i] - 1, 0)
            s_vmem[i] = total + jnp.where(plan[3, i] > 0, sums[last], 0.0)

    def forward(step, e):
        other = partner(me, step, groups)
        return pltpu.make_async_remote_copy(
            src_ref=landed.at[other],
            dst_ref=far.at[mine, other],
            send_sem=pass_send.at[e - 1, step],
            recv_sem=pass_recv.at[e - 1, step],
            device_id=(me, (mine + e) % shards),
            device_id_type=MESH,
        )

    def order(i):
        return i

    def arrived(i, carry):
        step = order(i)

        boundary(step).wait_recv()
        for e in range(1, shards):
            forward(step, e).start()
        return carry

    def moved(i):
        step = order(i)
        other = partner(me, step, groups)
        found = plan[1, other]
        t = jnp.minimum(found, tiles - 1)
        relation = tile_relation[0, t]
        value = jnp.dot(
            landed[other], w_all[mine, relation], preferred_element_type=jnp.float32
        )
        for e in range(1, shards):
            origin = (mine + shards - e) % shards
            pltpu.make_async_remote_copy(
                src_ref=far.at[origin, other],
                dst_ref=far.at[origin, other],
                send_sem=pass_send.at[e - 1, step],
                recv_sem=pass_recv.at[e - 1, step],
                device_id=(me, (mine + e) % shards),
                device_id_type=MESH,
            ).wait_recv()
            value = value + jnp.dot(
                far[origin, other], w_all[origin, relation], preferred_element_type=jnp.float32
            )
        value = value.astype(coef.dtype)
        result = jnp.dot(coef[t], value, preferred_element_type=jnp.float32)
        return result, jnp.where(found < tiles, tile_target[0, t], -1)

    def merge(step, carry):
        result, target = moved(step)
        for i in range(blocks):
            s_vmem[i] = s_vmem[i] + jnp.where(target == i, result, 0.0)
        return carry

    def serve(i, carry):
        arrived(i, carry)
        return merge(i - 1, carry)

    def told(step, carry):
        flagged(step).wait()
        return carry

    flag_copy = pltpu.make_async_copy(flag_vmem, flag_out, table_sem.at[1])
    with jax.named_scope("arrive"):
        lax.fori_loop(1, groups, told, 0)
        flag_vmem[...] = jnp.max(flags[...], axis=0)
        lax.fori_loop(1, 2 * plane, arrived, 0)
    with jax.named_scope("merge"):
        lax.fori_loop(1, 2 * plane - 1, merge, 0)
    flag_copy.start()
    with jax.named_scope("serve"):
        lax.fori_loop(2 * plane, groups - 1, serve, 0)
    with jax.named_scope("last"):
        arrived(groups - 1, 0)
    with jax.named_scope("lastm"):
        merge(groups - 2, 0)
    with jax.named_scope("lastmv"):
        result, target = moved(groups - 1)
        for i in range(blocks):
            value = s_vmem[i] + jnp.where(target == i, result, 0.0)
            pre_out[i] = jnp.maximum(value, 0.0).astype(pre_out.dtype)

    def finish(step, carry):
        for e in range(1, shards):
            forward(step, e).wait_send()
        return carry

    def finish_send(step, carry):
        boundary(step).wait_send()
        return carry

    with jax.named_scope("finish"):
        lax.fori_loop(1, groups, finish, 0)
        lax.fori_loop(1, groups, finish_send, 0)
        flag_copy.wait()


def store_kernel(x_ref, out_hbm, sem):
    copy = pltpu.make_async_copy(x_ref, out_hbm, sem)
    copy.start()
    copy.wait()


def tile_kernel(
    tile_source,
    tile_target,
    tile_relation,
    coef_hbm,
    pre_hbm,
    received,
    w_hbm,
    out_hbm,
    coef,
    x_tiles,
    w_vmem,
    total,
    pre,
    result,
    seen,
    sems,
):
    tiles = tile_source.shape[1]
    shards, groups = received.shape[:2]
    own = result.shape[0]
    ins = [pltpu.make_async_copy(pre_hbm.at[i], pre.at[i], sems.at[i]) for i in range(own)]
    outs = [
        pltpu.make_async_copy(result.at[i], out_hbm.at[i], sems.at[own + i]) for i in range(own)
    ]
    for copy in ins:
        copy.start()
    for s in range(groups):
        seen[s] = 0

    def look(t, count):
        source = tile_source[0, t] - own

        def repeated():
            before = seen[source]
            seen[source] = 1
            return count + before

        return lax.cond(source >= 0, repeated, lambda: count)

    count = lax.fori_loop(0, tiles, look, 0)

    @pl.when(count == 0)
    def _():
        for i in range(own):
            ins[i].wait()
            result[i] = jnp.maximum(pre[i].astype(jnp.float32), 0.0).astype(result.dtype)
            if i > 0:
                outs[i - 1].start()

    @pl.when(count > 0)
    def _():
        for i in range(own):
            ins[i].wait()
            total[i] = pre[i].astype(jnp.float32)
        for s in range(groups):
            seen[s] = 0

        def add(t, carry):
            source = tile_source[0, t] - own

            @pl.when(source >= 0)
            def _():
                before = seen[source]
                seen[source] = 1

                @pl.when(before == 1)
                def _():
                    copies = [
                        pltpu.make_async_copy(received.at[:, source], x_tiles, sems.at[2 * own]),
                        pltpu.make_async_copy(
                            w_hbm.at[:, tile_relation[0, t]], w_vmem, sems.at[2 * own + 1]
                        ),
                        pltpu.make_async_copy(coef_hbm.at[t], coef, sems.at[2 * own + 2]),
                    ]
                    for copy in copies:
                        copy.start()
                    for copy in copies:
                        copy.wait()
                    value = jnp.dot(x_tiles[0], w_vmem[0], preferred_element_type=jnp.float32)
                    for e in range(1, shards):
                        value = value + jnp.dot(
                            x_tiles[e], w_vmem[e], preferred_element_type=jnp.float32
                        )
                    total[tile_target[0, t]] += jnp.dot(
                        coef[...], value.astype(coef.dtype), preferred_element_type=jnp.float32
                    )

            return carry

        lax.fori_loop(0, tiles, add, 0)
        for i in range(own):
            result[i] = jnp.maximum(total[i], 0.0).astype(result.dtype)
            if i > 0:
                outs[i - 1].start()

    outs[-1].start()
    for copy in outs:
        copy.wait()


def per_device(
    groups,
    shards,
    features,
    rel_weight,
    self_weight,
    type_bias,
    node_type,
    tile_coef,
    tile_source,
    tile_target,
    tile_relation,
    send_block,
    send_live,
):
    rows, width = features.shape
    tiles, block, _ = tile_coef.shape
    relations = rel_weight.shape[0]
    kind = features.dtype
    smem = pl.BlockSpec(memory_space=pltpu.SMEM)
    vmem = pl.BlockSpec(memory_space=pltpu.VMEM)
    anywhere = pl.BlockSpec(memory_space=pl.ANY)
    hbm = pl.BlockSpec(memory_space=pltpu.HBM)
    dma = pltpu.SemaphoreType.DMA
    blocks = rows // block
    lanes = 128 * pl.cdiv(max(tiles, groups, blocks), 128)
    plane = groups // 4
    capacity = 3 * blocks // 4 if 2 * plane <= blocks else blocks
    wide = (1, 128)
    operands = (
        send_block,
        send_live,
        tile_source,
        tile_target,
        tile_relation,
        type_bias,
        node_type.reshape(blocks, block),
        features.reshape(blocks, block, width),
        rel_weight,
        self_weight,
        tile_coef,
    )
    def dense():
        received, weights, pre = pl.pallas_call(
            functools.partial(exchange_kernel, groups, shards, block),
            out_shape=(
                jax.ShapeDtypeStruct((shards, groups, block, width), kind),
                jax.ShapeDtypeStruct((shards, relations, width, width), kind),
                jax.ShapeDtypeStruct((blocks, block, width), kind),
            ),
            in_specs=[anywhere] * 11,
            out_specs=(anywhere,) * 3,
            scratch_shapes=[
                pltpu.VMEM((groups, block, width), kind),
                pltpu.VMEM((blocks, block, width), kind),
                pltpu.VMEM((shards, blocks, block, width), kind),
                pltpu.VMEM((shards, relations + 1, width, width), kind),
                pltpu.VMEM((blocks, block, width), jnp.float32),
                pltpu.VMEM((tiles, block, block), kind),
                pltpu.VMEM((tiles, block, width), jnp.float32),
                pltpu.VMEM((groups, block, width), kind),
                pltpu.VMEM((shards, groups, block, width), kind),
                pltpu.VMEM((blocks, block, width), kind),
                pltpu.VMEM((8, lanes), jnp.int32),
                pltpu.SMEM((8, lanes), jnp.int32),
                pltpu.SMEM(send_block.shape, jnp.int32),
                pltpu.SMEM(send_block.shape, jnp.int32),
                pltpu.SMEM(tile_source.shape, jnp.int32),
                pltpu.SMEM(tile_source.shape, jnp.int32),
                pltpu.SMEM(tile_source.shape, jnp.int32),
                pltpu.VMEM(tile_source.shape, jnp.int32),
                pltpu.VMEM(tile_source.shape, jnp.int32),
                pltpu.VMEM(type_bias.shape, jnp.float32),
                pltpu.VMEM((blocks, block), jnp.int32),
                dma((9,)),
                dma((groups,)),
                dma((groups,)),
                dma((max(shards - 1, 1), groups)),
                dma((max(shards - 1, 1), groups)),
                dma((max(shards - 1, 1), 3)),
                dma((max(shards - 1, 1), 3)),
                dma((6,)),
                dma((groups,)),
                dma((max(shards - 1, 1), groups)),
                dma((blocks,)),
            ],
            compiler_params=pltpu.CompilerParams(
                collective_id=1, has_side_effects=True, vmem_limit_bytes=VMEM
            ),
            name="exchange",
        )(*operands)
        updated = pl.pallas_call(
            tile_kernel,
            out_shape=jax.ShapeDtypeStruct((blocks, block, width), kind),
            in_specs=[smem] * 3 + [anywhere] * 4,
            out_specs=anywhere,
            scratch_shapes=[
                pltpu.VMEM((block, block), kind),
                pltpu.VMEM((shards, block, width), kind),
                pltpu.VMEM((shards, width, width), kind),
                pltpu.VMEM((blocks, block, width), jnp.float32),
                pltpu.VMEM((blocks, block, width), kind),
                pltpu.VMEM((blocks, block, width), kind),
                pltpu.SMEM((groups,), jnp.int32),
                dma((2 * blocks + 3,)),
            ],
            compiler_params=pltpu.CompilerParams(vmem_limit_bytes=VMEM),
            name="tiles",
        )(tile_source, tile_target, tile_relation, tile_coef, pre, received, weights)
        return updated

    result, flag = pl.pallas_call(
        functools.partial(relay_kernel, groups, shards, block),
        out_shape=(
            jax.ShapeDtypeStruct((blocks, block, width), kind),
            jax.ShapeDtypeStruct((1, 128), jnp.int32),
        ),
        in_specs=[hbm] * 11,
        out_specs=(vmem, hbm),
        scratch_shapes=[
            pltpu.VMEM((groups, block, width), kind),
            pltpu.VMEM((blocks, block, width), kind),
            pltpu.VMEM((shards, blocks, block, width), kind),
            pltpu.VMEM((shards, relations + 1, width, width), kind),
            pltpu.VMEM((blocks, block, width), jnp.float32),
            pltpu.VMEM((tiles, block, block), kind),
            pltpu.VMEM((tiles, block, width), jnp.float32),
            pltpu.VMEM((groups, block, width), kind),
            pltpu.VMEM((shards, groups, block, width), kind),
            pltpu.VMEM((capacity, block, width), kind),
            pltpu.VMEM((capacity, block, width), kind),
            pltpu.VMEM((2 * plane, block, width), kind),
            pltpu.VMEM((2 * plane, 128), jnp.int32),
            pltpu.VMEM((2 * plane, 128), jnp.int32),
            pltpu.SMEM((2 * plane, 128), jnp.int32),
            pltpu.VMEM((groups, 1, 128), jnp.int32),
            pltpu.VMEM((1, 128), jnp.int32),
            pltpu.VMEM((8, lanes), jnp.int32),
            pltpu.SMEM((8, lanes), jnp.int32),
            pltpu.SMEM(send_block.shape, jnp.int32),
            pltpu.SMEM(send_block.shape, jnp.int32),
            pltpu.SMEM(tile_source.shape, jnp.int32),
            pltpu.SMEM(tile_source.shape, jnp.int32),
            pltpu.SMEM(tile_source.shape, jnp.int32),
            pltpu.VMEM(tile_source.shape, jnp.int32),
            pltpu.VMEM(tile_source.shape, jnp.int32),
            pltpu.VMEM(type_bias.shape, jnp.float32),
            pltpu.VMEM((blocks, block), jnp.int32),
            dma((9,)),
            dma((groups,)),
            dma((groups,)),
            dma((max(shards - 1, 1), groups)),
            dma((max(shards - 1, 1), groups)),
            dma((max(shards - 1, 1), 3)),
            dma((max(shards - 1, 1), 3)),
            dma((6,)),
            dma((capacity + 1,)),
            dma((capacity + 1,)),
            dma((2 * plane,)),
            dma((groups,)),
            dma((groups,)),
            dma((2,)),
        ],
        compiler_params=pltpu.CompilerParams(
            collective_id=0, has_side_effects=True, vmem_limit_bytes=56 << 20
        ),
        name="relay",
    )(*operands)

    def store():
        return pl.pallas_call(
            store_kernel,
            out_shape=jax.ShapeDtypeStruct((blocks, block, width), kind),
            in_specs=[vmem],
            out_specs=hbm,
            scratch_shapes=[dma(())],
            compiler_params=pltpu.CompilerParams(vmem_limit_bytes=2 << 20),
            name="store",
        )(result)

    updated = lax.cond(flag[0, 0] > 0, dense, store)
    return updated.reshape(rows, width)


def solution(mesh):
    placed = (
        P("graph", "feat"),
        P(None, "feat", None),
        P("feat", None),
        P(None, "feat"),
        P("graph"),
        P("graph", None, None),
        P("graph", None),
        P("graph", None),
        P("graph", None),
        P("graph", None),
        P("graph", None),
    )
    groups, shards = mesh.shape["graph"], mesh.shape["feat"]
    return jax.shard_map(
        functools.partial(per_device, groups, shards),
        mesh=mesh,
        in_specs=placed,
        out_specs=P("graph", "feat"),
        check_vma=False,
    )
```
